32 devices in a mesh: batch: 8 (over z, y), mp: 4 (over x, core).
Axes of the slice: x: 2, y: 2, z: 4, core: 2. Of those that a mesh axis runs over, the one named last changes fastest.
Arguments:
- lookup_ids: int32 [64, 16384], P('batch'), may hold values from 0 to 8191
- table_feature: int32 [64], replicated, may hold values from 0 to 63, each once
- tables: bfloat16 [64, 8192, 128], P('batch'), may hold values from -6 to 6
- cross_down: bfloat16 [2, 8192, 512], P(None, 'mp'), may hold values from -0.0625 to 0.0625
- cross_up: bfloat16 [2, 512, 8192], P(None, None, 'mp'), may hold values from -0.25 to 0.25
- cross_bias: float32 [2, 8192], P(None, 'mp'), may hold values from -3 to 3
Outputs:
- crossed: bfloat16 [16384, 8192], P('batch', 'mp')
The draws below stay inside these ranges and needn't reach their ends.
Inputs may be any that keep to these rules, and one draw needn't show every extreme that they name: `table_feature`: each number appears once.
All inputs are finite; a program needn't handle non-finite values.
Results may differ from the reference program's by a relative error of at most 0.015.
Values may be sent and summed in bfloat16 or wider, within the bound.
A program may use at most 128 MiB of HBM per device.

```python
import math
import jax
import jax.numpy as jnp
import numpy as np
from jax import lax

FEATS = 64
EMB = 128
RANK = 512
ROWS = 8192
LAYERS = 2
WIDTH = 8192
BATCH = 16384
N_MP = 4


def plant(drawn, stream_key, low, top_value):
    place = [jax.random.randint(jax.random.fold_in(stream_key, axis), (), 0, length) for axis, length in enumerate(drawn.shape)]
    main_axis = drawn.shape.index(max(drawn.shape))
    neighbour = place[:main_axis] + [(place[main_axis] + 1) % drawn.shape[main_axis]] + place[main_axis + 1:]
    return drawn.at[tuple(place)].set(low).at[tuple(neighbour)].set(top_value)


def shard_levels(own_key, dims, pieces, low, high):
    factor_of = 1.0
    for axis_at, blocks in pieces:
        draws = jax.random.uniform(jax.random.fold_in(jax.random.fold_in(own_key, 6), axis_at), (blocks,), jnp.float32, low / len(pieces), high / len(pieces))
        factor_of = factor_of * jnp.repeat(jnp.exp(draws), dims[axis_at] // blocks).reshape((-1,) + (1,) * (len(dims) - 1 - axis_at))
    return factor_of


def rank_table(number_of, slope):
    weights = [(1 << 20) // math.isqrt(rank ** slope) + 1 for rank in range(1, number_of + 1)]
    width = 1 + sum(weights) // (1 << 30)
    return np.cumsum(np.array([max(1, weight // width) for weight in weights]))


def skewed_ids(stream_key, shape, amount, slope):
    grid = rank_table(amount, slope)
    lot = jax.random.randint(jax.random.fold_in(stream_key, 1), shape, 0, int(grid[amount - 1]))
    standing = jnp.searchsorted(jnp.asarray(grid, jnp.int32), lot, side="right")
    return jax.random.permutation(jax.random.fold_in(stream_key, 2), amount)[standing].astype(jnp.int32)


def centred(key, extent, width, bound, cuts=(), held_as=jnp.bfloat16):
    values = jax.random.normal(key, extent, jnp.float32) * width
    if len(cuts) > 0:
        values = shard_levels(key, extent, cuts, -0.22, 0.18) * values
    return jnp.clip(values, min=-bound, max=bound).astype(held_as)


def setup_inputs(seed: int = 0) -> dict:
    streams_of = jax.random.split(jax.random.key(seed), 7)
    lookup_ids = plant(skewed_ids(streams_of[0], (FEATS, BATCH), ROWS, 2), jax.random.fold_in(streams_of[0], 3), 0, ROWS - 1).astype(jnp.int32)
    table_feature = jax.random.permutation(streams_of[1], FEATS).astype(jnp.int32)
    tables = centred(streams_of[2], (FEATS, ROWS, EMB), 1.0, 6.0, ((0, 8),))
    cross_down = centred(streams_of[3], (LAYERS, WIDTH, RANK), WIDTH ** -0.5, 0.0625, ((1, 4),))
    cross_up = centred(streams_of[4], (LAYERS, RANK, WIDTH), RANK ** -0.5, 0.25, ((2, 4),))
    cross_bias = centred(streams_of[5], (LAYERS, WIDTH), 0.5, 3.0, ((1, 4),), jnp.float32)
    return dict(lookup_ids=lookup_ids, table_feature=table_feature, tables=tables, cross_down=cross_down, cross_up=cross_up, cross_bias=cross_bias)


def reference(lookup_ids, table_feature, tables, cross_down, cross_up, cross_bias):
    looked = jax.vmap(lambda table, index: jnp.take(table, index, axis=0))(tables, lookup_ids)
    inverse = jnp.zeros((FEATS,), jnp.int32).at[table_feature].set(jnp.arange(FEATS, dtype=jnp.int32))
    by_feature = jnp.take(looked, inverse, axis=0)
    embedded = jnp.transpose(by_feature, (1, 2, 0)).reshape(BATCH, EMB * FEATS)
    block = WIDTH // N_MP
    state = embedded
    for layer in range(LAYERS):
        low_sum = jnp.zeros((BATCH, RANK), jnp.float32)
        for piece in range(N_MP):
            term = jnp.dot(state[:, piece * block:(piece + 1) * block], cross_down[layer, piece * block:(piece + 1) * block, :], preferred_element_type=jnp.float32)
            rounded = lax.optimization_barrier(term.astype(jnp.bfloat16))
            low_sum = low_sum + rounded.astype(jnp.float32)
        low = low_sum.astype(jnp.bfloat16)
        high = jnp.dot(low, cross_up[layer], preferred_element_type=jnp.float32) + cross_bias[layer][None, :]
        state = (embedded.astype(jnp.float32) * high + state.astype(jnp.float32)).astype(jnp.bfloat16)
    return state
```

```python
import functools

import jax
import jax.numpy as jnp
from jax import lax
from jax.experimental import pallas as pl
from jax.experimental.pallas import tpu as pltpu
from jax.sharding import PartitionSpec as P

MESH = pl.DeviceIdType.MESH
GROUP = 16


def gather_kernel(ids_ref, table_ref, out_ref, wide, rows):
    sources, groups, _, emb_local, share = out_ref.shape
    slot = pl.program_id(0)
    buckets = wide.shape[0]
    step = 256

    @pl.loop(0, buckets // step)
    def _(i):
        part = pl.ds(pl.multiple_of(i * step, step), step)
        wide[part, :] = table_ref[0, part, :].astype(jnp.float32)

    unroll = 32

    @pl.loop(0, sources)
    def _(dest):
        @pl.loop(0, share // unroll)
        def _(i):
            base = pl.multiple_of(i * unroll, unroll)
            for k in range(unroll):
                at = ids_ref[slot, dest * share + base + k]
                rows[pl.ds(base + k, 1), :] = wide[pl.ds(at, 1), :]

        turned = rows[...].T.astype(jnp.bfloat16)
        for m in range(groups):
            out_ref[dest, m, 0] = turned[m * emb_local : (m + 1) * emb_local]


def gather(wanted, tables, sources, groups, share):
    slots, buckets, emb = tables.shape
    emb_local = emb // groups
    return pl.pallas_call(
        gather_kernel,
        out_shape=jax.ShapeDtypeStruct((sources, groups, slots, emb_local, share), tables.dtype),
        grid_spec=pltpu.PrefetchScalarGridSpec(
            num_scalar_prefetch=1,
            grid=(slots,),
            in_specs=[pl.BlockSpec((1, buckets, emb), lambda s, ids: (s, 0, 0))],
            out_specs=pl.BlockSpec(
                (sources, groups, 1, emb_local, share), lambda s, ids: (0, 0, s, 0, 0)
            ),
            scratch_shapes=[
                pltpu.VMEM((buckets, emb), jnp.float32),
                pltpu.VMEM((share, emb), jnp.float32),
            ],
        ),
        compiler_params=pltpu.CompilerParams(vmem_limit_bytes=40 * 2**20),
        name="lookup",
    )(wanted, tables)


def partner(me, mask, size):
    other = me
    bit = 1
    while bit < size:
        if mask & bit:
            other = other + bit * (1 - 2 * ((me // bit) % 2))
        bit *= 2
    return other


def exchange_kernel(sources, groups, src_ref, dst_ref, send_sem, recv_sem, own_sem):
    b, m = lax.axis_index("batch"), lax.axis_index("mp")
    masks = [
        (x, y)
        for x in range(sources - 1, -1, -1)
        for y in range(groups - 1, -1, -1)
        if (x, y) != (0, 0)
    ]
    peers = [(partner(b, x, sources), partner(m, y, groups)) for x, y in masks]
    barrier = pltpu.get_barrier_semaphore()
    for peer in peers:
        pl.semaphore_signal(barrier, inc=1, device_id=peer, device_id_type=MESH)
    pl.semaphore_wait(barrier, len(peers))
    copies = []
    for k, peer in enumerate(peers):
        copy = pltpu.make_async_remote_copy(
            src_ref=src_ref.at[peer[0], peer[1]],
            dst_ref=dst_ref.at[b, m],
            send_sem=send_sem.at[k],
            recv_sem=recv_sem.at[k],
            device_id=peer,
            device_id_type=MESH,
        )
        copy.start()
        copies.append(copy)
    own = pltpu.make_async_copy(src_ref.at[b, m], dst_ref.at[b, m], own_sem)
    own.start()
    own.wait()
    for copy in copies:
        copy.wait()


def exchange(sent):
    sources, groups = sent.shape[:2]
    peers = sources * groups - 1
    return pl.pallas_call(
        functools.partial(exchange_kernel, sources, groups),
        out_shape=jax.ShapeDtypeStruct(sent.shape, sent.dtype),
        in_specs=[pl.BlockSpec(memory_space=pl.ANY)],
        out_specs=pl.BlockSpec(memory_space=pl.ANY),
        scratch_shapes=[
            pltpu.SemaphoreType.DMA((peers,)),
            pltpu.SemaphoreType.DMA((peers,)),
            pltpu.SemaphoreType.DMA,
        ],
        compiler_params=pltpu.CompilerParams(collective_id=0, has_side_effects=True),
        name="exchange",
    )(sent)


def place_kernel(x_ref, placing_ref, down_ref, emb_ref, term_ref, total):
    sources, _, slots, group, share = x_ref.shape
    j = pl.program_id(1)
    x = x_ref[...].reshape(sources * slots * group, share)
    emb = lax.dot_general(
        x, placing_ref[...], (((0,), (0,)), ((), ())), preferred_element_type=jnp.float32
    ).astype(jnp.bfloat16)
    emb_ref[...] = emb
    part = jnp.dot(emb, down_ref[0], preferred_element_type=jnp.float32)

    @pl.when(j == 0)
    def _():
        total[...] = part

    @pl.when(j > 0)
    def _():
        total[...] += part

    @pl.when(j == pl.num_programs(1) - 1)
    def _():
        term_ref[...] = total[...].astype(jnp.bfloat16)


def place(received, placing, cross_down):
    sources, groups, slots, emb_local, share = received.shape
    _, width, rank = cross_down.shape
    cols = sources * slots * GROUP
    return pl.pallas_call(
        place_kernel,
        out_shape=(
            jax.ShapeDtypeStruct((groups * share, width), jnp.bfloat16),
            jax.ShapeDtypeStruct((groups * share, rank), jnp.bfloat16),
        ),
        grid=(groups, emb_local // GROUP),
        in_specs=[
            pl.BlockSpec((sources, 1, slots, GROUP, share), lambda i, j: (0, i, 0, j, 0)),
            pl.BlockSpec((cols, cols), lambda i, j: (0, 0)),
            pl.BlockSpec((1, cols, rank), lambda i, j: (0, j, 0)),
        ],
        out_specs=(
            pl.BlockSpec((share, cols), lambda i, j: (i, j)),
            pl.BlockSpec((share, rank), lambda i, j: (i, 0)),
        ),
        scratch_shapes=[pltpu.VMEM((share, rank), jnp.float32)],
        compiler_params=pltpu.CompilerParams(vmem_limit_bytes=40 * 2**20),
        name="place",
    )(received, placing, cross_down)


def per_device(lookup_ids, table_feature, tables, cross_down, cross_up, cross_bias):
    slots_local = tables.shape[0]
    feats = table_feature.shape[0]
    sources = lax.axis_size("batch")
    groups = lax.axis_size("mp")
    examples_local = lookup_ids.shape[1] // sources
    share = examples_local // groups
    start = lax.axis_index("mp") * share
    by_owner = lookup_ids.reshape(slots_local, sources, examples_local)
    wanted = lax.dynamic_slice_in_dim(by_owner, start, share, 2)
    wanted = wanted.reshape(slots_local, sources * share)
    received = exchange(gather(wanted, tables, sources, groups, share))
    fits = table_feature[:, None] == jnp.arange(feats, dtype=jnp.int32)[None, :]
    same = jnp.arange(GROUP)[:, None] == jnp.arange(GROUP)[None, :]
    placing = (
        (fits[:, None, None, :] & same[None, :, :, None])
        .reshape(feats * GROUP, GROUP * feats)
        .astype(jnp.bfloat16)
    )
    embedded, term = place(received, placing, cross_down)
    embedded_wide = embedded.astype(jnp.float32)
    state = embedded
    for layer in range(len(cross_down)):
        if layer > 0:
            term = jnp.dot(state, cross_down[layer], preferred_element_type=jnp.float32)
            term = term.astype(jnp.bfloat16)
        low = lax.psum(term, "mp")
        high = (
            jnp.dot(low, cross_up[layer], preferred_element_type=jnp.float32)
            + cross_bias[layer][None, :]
        )
        state = (embedded_wide * high + state.astype(jnp.float32)).astype(jnp.bfloat16)
    return state


def solution(mesh):
    return jax.shard_map(
        per_device,
        mesh=mesh,
        in_specs=(
            P("batch", None),
            P(),
            P("batch", None, None),
            P(None, "mp", None),
            P(None, None, "mp"),
            P(None, "mp"),
        ),
        out_specs=P("batch", "mp"),
        check_vma=False,
    )
```

```python
import functools

import jax
import jax.numpy as jnp
from jax import lax
from jax.experimental import pallas as pl
from jax.experimental.pallas import tpu as pltpu
from jax.sharding import PartitionSpec as P

MESH = pl.DeviceIdType.MESH
GROUP = 16


def gather_kernel(ids_ref, table_ref, out_ref, wide, rows):
    sources, groups, _, emb_local, share = out_ref.shape
    slot = pl.program_id(0)
    buckets = wide.shape[0]
    step = 256

    @pl.loop(0, buckets // step)
    def _(i):
        part = pl.ds(pl.multiple_of(i * step, step), step)
        wide[part, :] = table_ref[0, part, :].astype(jnp.float32)

    unroll = 32

    @pl.loop(0, sources)
    def _(dest):
        @pl.loop(0, share // unroll)
        def _(i):
            base = pl.multiple_of(i * unroll, unroll)
            for k in range(unroll):
                at = ids_ref[slot, dest * share + base + k]
                rows[pl.ds(base + k, 1), :] = wide[pl.ds(at, 1), :]

        turned = rows[...].T.astype(jnp.bfloat16)
        for m in range(groups):
            out_ref[dest, m, 0] = turned[m * emb_local : (m + 1) * emb_local]


def gather(wanted, tables, sources, groups, share):
    slots, buckets, emb = tables.shape
    emb_local = emb // groups
    return pl.pallas_call(
        gather_kernel,
        out_shape=jax.ShapeDtypeStruct((sources, groups, slots, emb_local, share), tables.dtype),
        grid_spec=pltpu.PrefetchScalarGridSpec(
            num_scalar_prefetch=1,
            grid=(slots,),
            in_specs=[pl.BlockSpec((1, buckets, emb), lambda s, ids: (s, 0, 0))],
            out_specs=pl.BlockSpec(
                (sources, groups, 1, emb_local, share), lambda s, ids: (0, 0, s, 0, 0)
            ),
            scratch_shapes=[
                pltpu.VMEM((buckets, emb), jnp.float32),
                pltpu.VMEM((share, emb), jnp.float32),
            ],
        ),
        compiler_params=pltpu.CompilerParams(vmem_limit_bytes=40 * 2**20),
        name="lookup",
    )(wanted, tables)


def partner(me, mask, size):
    other = me
    bit = 1
    while bit < size:
        if mask & bit:
            other = other + bit * (1 - 2 * ((me // bit) % 2))
        bit *= 2
    return other


def exchange_kernel(sources, groups, src_ref, dst_ref, send_sem, recv_sem, own_sem):
    b, m = lax.axis_index("batch"), lax.axis_index("mp")
    masks = [
        (x, y)
        for x in range(sources - 1, -1, -1)
        for y in range(groups - 1, -1, -1)
        if (x, y) != (0, 0)
    ]
    peers = [(partner(b, x, sources), partner(m, y, groups)) for x, y in masks]
    barrier = pltpu.get_barrier_semaphore()
    for peer in peers:
        pl.semaphore_signal(barrier, inc=1, device_id=peer, device_id_type=MESH)
    pl.semaphore_wait(barrier, len(peers))
    copies = []
    for k, peer in enumerate(peers):
        copy = pltpu.make_async_remote_copy(
            src_ref=src_ref.at[peer[0], peer[1]],
            dst_ref=dst_ref.at[b, m],
            send_sem=send_sem.at[k],
            recv_sem=recv_sem.at[k],
            device_id=peer,
            device_id_type=MESH,
        )
        copy.start()
        copies.append(copy)
    own = pltpu.make_async_copy(src_ref.at[b, m], dst_ref.at[b, m], own_sem)
    own.start()
    own.wait()
    for copy in copies:
        copy.wait()


def exchange(sent):
    sources, groups = sent.shape[:2]
    peers = sources * groups - 1
    return pl.pallas_call(
        functools.partial(exchange_kernel, sources, groups),
        out_shape=jax.ShapeDtypeStruct(sent.shape, sent.dtype),
        in_specs=[pl.BlockSpec(memory_space=pl.ANY)],
        out_specs=pl.BlockSpec(memory_space=pl.ANY),
        scratch_shapes=[
            pltpu.SemaphoreType.DMA((peers,)),
            pltpu.SemaphoreType.DMA((peers,)),
            pltpu.SemaphoreType.DMA,
        ],
        compiler_params=pltpu.CompilerParams(collective_id=0, has_side_effects=True),
        name="exchange",
    )(sent)


def place_kernel(x_ref, column_ref, down_ref, emb_ref, term_ref, placing_ref, total):
    sources, _, slots, group, share = x_ref.shape
    i, j = pl.program_id(0), pl.program_id(1)

    @pl.when((i == 0) & (j == 0))
    def _():
        columns = lax.broadcasted_iota(jnp.int32, placing_ref.shape, 1)
        placing_ref[...] = jnp.where(column_ref[...] == columns, 1.0, 0.0).astype(jnp.bfloat16)

    x = x_ref[...].reshape(sources * slots * group, share)
    emb = lax.dot_general(
        x, placing_ref[...], (((0,), (0,)), ((), ())), preferred_element_type=jnp.float32
    ).astype(jnp.bfloat16)
    emb_ref[...] = emb
    part = jnp.dot(emb, down_ref[0], preferred_element_type=jnp.float32)

    @pl.when(j == 0)
    def _():
        total[...] = part

    @pl.when(j > 0)
    def _():
        total[...] += part

    @pl.when(j == pl.num_programs(1) - 1)
    def _():
        term_ref[...] = total[...].astype(jnp.bfloat16)


def place(received, column, cross_down):
    sources, groups, slots, emb_local, share = received.shape
    _, width, rank = cross_down.shape
    cols = sources * slots * GROUP
    return pl.pallas_call(
        place_kernel,
        out_shape=(
            jax.ShapeDtypeStruct((groups * share, width), jnp.bfloat16),
            jax.ShapeDtypeStruct((groups * share, rank), jnp.bfloat16),
        ),
        grid=(groups, emb_local // GROUP),
        in_specs=[
            pl.BlockSpec((sources, 1, slots, GROUP, share), lambda i, j: (0, i, 0, j, 0)),
            pl.BlockSpec((cols, 1), lambda i, j: (0, 0)),
            pl.BlockSpec((1, cols, rank), lambda i, j: (0, j, 0)),
        ],
        out_specs=(
            pl.BlockSpec((share, cols), lambda i, j: (i, j)),
            pl.BlockSpec((share, rank), lambda i, j: (i, 0)),
        ),
        scratch_shapes=[
            pltpu.VMEM((cols, cols), jnp.bfloat16),
            pltpu.VMEM((share, rank), jnp.float32),
        ],
        compiler_params=pltpu.CompilerParams(vmem_limit_bytes=40 * 2**20),
        name="place",
    )(received, column, cross_down)


PIECES = 4


def reduce_kernel(groups, term_ref, low_ref, near_in, held, far_in, *sems):
    b, m = lax.axis_index("batch"), lax.axis_index("mp")
    near_send, near_recv, far_send, far_recv, back_send, back_recv = sems
    near = (b, partner(m, 1, groups))
    far = [(b, partner(m, 1 << (s + 1), groups)) for s in range(far_in.shape[0])]
    half = term_ref.shape[0] // 2
    piece = half // PIECES
    core = m % 2

    def rows(who, k):
        return pl.ds(pl.multiple_of(who * half + k * piece, piece), piece)

    barrier = pltpu.get_barrier_semaphore()
    for peer in [near] + far:
        pl.semaphore_signal(barrier, inc=1, device_id=peer, device_id_type=MESH)
    pl.semaphore_wait(barrier, 1 + len(far))

    def send(src, dst, send_sem, recv_sem, peer):
        copy = pltpu.make_async_remote_copy(
            src_ref=src,
            dst_ref=dst,
            send_sem=send_sem,
            recv_sem=recv_sem,
            device_id=peer,
            device_id_type=MESH,
        )
        copy.start()
        return copy

    sent = []
    going = [
        send(term_ref.at[rows(1 - core, k)], near_in.at[k], near_send.at[k], near_recv.at[k], near)
        for k in range(PIECES)
    ]
    for s in range(len(far) + 1):
        arriving, going = going, []
        for k in range(PIECES):
            arriving[k].wait_recv()
            if s == 0:
                mine, other = term_ref[rows(core, k)], near_in[k]
            else:
                mine, other = held[s - 1, k], far_in[s - 1, k]
            total = (mine.astype(jnp.float32) + other.astype(jnp.float32)).astype(jnp.bfloat16)
            if s < len(far):
                held[s, k] = total
                going.append(
                    send(
                        held.at[s, k], far_in.at[s, k], far_send.at[s, k], far_recv.at[s, k], far[s]
                    )
                )
            else:
                place = rows(core, k)
                low_ref[place] = total
                going.append(
                    send(low_ref.at[place], low_ref.at[place], back_send.at[k], back_recv.at[k], near)
                )
        sent += arriving
    for copy in going:
        copy.wait_recv()
    for copy in sent + going:
        copy.wait_send()


def reduce_over_mp(term):
    groups = lax.axis_size("mp")
    stages = groups.bit_length() - 2
    rows, rank = term.shape
    block = (PIECES, rows // 2 // PIECES, rank)
    dma = pltpu.SemaphoreType.DMA
    return pl.pallas_call(
        functools.partial(reduce_kernel, groups),
        out_shape=jax.ShapeDtypeStruct(term.shape, term.dtype),
        in_specs=[pl.BlockSpec(memory_space=pltpu.VMEM)],
        out_specs=pl.BlockSpec(memory_space=pltpu.VMEM),
        scratch_shapes=[
            pltpu.VMEM(block, term.dtype),
            pltpu.VMEM((stages,) + block, term.dtype),
            pltpu.VMEM((stages,) + block, term.dtype),
            dma((PIECES,)),
            dma((PIECES,)),
            dma((stages, PIECES)),
            dma((stages, PIECES)),
            dma((PIECES,)),
            dma((PIECES,)),
        ],
        compiler_params=pltpu.CompilerParams(
            collective_id=1, has_side_effects=True, vmem_limit_bytes=24 * 2**20
        ),
        name="reduce",
    )(term)


def per_device(lookup_ids, table_feature, tables, cross_down, cross_up, cross_bias):
    slots_local = tables.shape[0]
    feats = table_feature.shape[0]
    sources = lax.axis_size("batch")
    groups = lax.axis_size("mp")
    examples_local = lookup_ids.shape[1] // sources
    share = examples_local // groups
    start = lax.axis_index("mp") * share
    by_owner = lookup_ids.reshape(slots_local, sources, examples_local)
    wanted = lax.dynamic_slice_in_dim(by_owner, start, share, 2)
    wanted = wanted.reshape(slots_local, sources * share)
    received = exchange(gather(wanted, tables, sources, groups, share))
    column = (table_feature[:, None] + feats * jnp.arange(GROUP)[None, :]).reshape(-1, 1)
    embedded, term = place(received, column, cross_down)
    embedded_wide = embedded.astype(jnp.float32)
    state = embedded
    for layer in range(len(cross_down)):
        if layer > 0:
            term = jnp.dot(state, cross_down[layer], preferred_element_type=jnp.float32)
            term = term.astype(jnp.bfloat16)
        low = reduce_over_mp(term)
        high = (
            jnp.dot(low, cross_up[layer], preferred_element_type=jnp.float32)
            + cross_bias[layer][None, :]
        )
        state = (embedded_wide * high + state.astype(jnp.float32)).astype(jnp.bfloat16)
    return state


def solution(mesh):
    return jax.shard_map(
        per_device,
        mesh=mesh,
        in_specs=(
            P("batch", None),
            P(),
            P("batch", None, None),
            P(None, "mp", None),
            P(None, None, "mp"),
            P(None, "mp"),
        ),
        out_specs=P("batch", "mp"),
        check_vma=False,
    )
```

```python
import functools

import jax
import jax.numpy as jnp
from jax import lax
from jax.experimental import pallas as pl
from jax.experimental.pallas import tpu as pltpu
from jax.sharding import PartitionSpec as P

MESH = pl.DeviceIdType.MESH
GROUP = 16


def gather_kernel(ids_ref, table_ref, out_ref, wide, rows):
    sources, groups, _, emb_local, share = out_ref.shape
    slot = pl.program_id(0)
    buckets = wide.shape[0]
    step = 256

    @pl.loop(0, buckets // step)
    def _(i):
        part = pl.ds(pl.multiple_of(i * step, step), step)
        wide[part, :] = table_ref[0, part, :].astype(jnp.float32)

    unroll = 32

    @pl.loop(0, sources)
    def _(dest):
        @pl.loop(0, share // unroll)
        def _(i):
            base = pl.multiple_of(i * unroll, unroll)
            first = (slot * sources + dest) * share + base
            for k in range(unroll):
                at = ids_ref[first + k]
                rows[pl.ds(base + k, 1), :] = wide[pl.ds(at, 1), :]

        turned = rows[...].T.astype(jnp.bfloat16)
        for m in range(groups):
            out_ref[dest, m, 0] = turned[m * emb_local : (m + 1) * emb_local]


def gather(wanted, tables, sources, groups, share):
    slots, buckets, emb = tables.shape
    emb_local = emb // groups
    return pl.pallas_call(
        gather_kernel,
        out_shape=jax.ShapeDtypeStruct((sources, groups, slots, emb_local, share), tables.dtype),
        grid_spec=pltpu.PrefetchScalarGridSpec(
            num_scalar_prefetch=1,
            grid=(slots,),
            in_specs=[pl.BlockSpec((1, buckets, emb), lambda s, ids: (s, 0, 0))],
            out_specs=pl.BlockSpec(
                (sources, groups, 1, emb_local, share), lambda s, ids: (0, 0, s, 0, 0)
            ),
            scratch_shapes=[
                pltpu.VMEM((buckets, emb), jnp.float32),
                pltpu.VMEM((share, emb), jnp.float32),
            ],
        ),
        compiler_params=pltpu.CompilerParams(vmem_limit_bytes=40 * 2**20),
        name="lookup",
    )(wanted, tables)


def partner(me, mask, size):
    other = me
    bit = 1
    while bit < size:
        if mask & bit:
            other = other + bit * (1 - 2 * ((me // bit) % 2))
        bit *= 2
    return other


def exchange_kernel(sources, groups, src_ref, dst_ref, send_sem, recv_sem, own_sem):
    b, m = lax.axis_index("batch"), lax.axis_index("mp")
    masks = [
        (x, y)
        for x in range(sources - 1, -1, -1)
        for y in range(groups - 1, -1, -1)
        if (x, y) != (0, 0)
    ]
    peers = [(partner(b, x, sources), partner(m, y, groups)) for x, y in masks]
    barrier = pltpu.get_barrier_semaphore()
    for peer in peers:
        pl.semaphore_signal(barrier, inc=1, device_id=peer, device_id_type=MESH)
    pl.semaphore_wait(barrier, len(peers))
    copies = []
    for k, peer in enumerate(peers):
        copy = pltpu.make_async_remote_copy(
            src_ref=src_ref.at[peer[0], peer[1]],
            dst_ref=dst_ref.at[b, m],
            send_sem=send_sem.at[k],
            recv_sem=recv_sem.at[k],
            device_id=peer,
            device_id_type=MESH,
        )
        copy.start()
        copies.append(copy)
    own = pltpu.make_async_copy(src_ref.at[b, m], dst_ref.at[b, m], own_sem)
    own.start()
    own.wait()
    for copy in copies:
        copy.wait()


def exchange(sent):
    sources, groups = sent.shape[:2]
    peers = sources * groups - 1
    return pl.pallas_call(
        functools.partial(exchange_kernel, sources, groups),
        out_shape=jax.ShapeDtypeStruct(sent.shape, sent.dtype),
        in_specs=[pl.BlockSpec(memory_space=pl.ANY)],
        out_specs=pl.BlockSpec(memory_space=pl.ANY),
        scratch_shapes=[
            pltpu.SemaphoreType.DMA((peers,)),
            pltpu.SemaphoreType.DMA((peers,)),
            pltpu.SemaphoreType.DMA,
        ],
        compiler_params=pltpu.CompilerParams(collective_id=0, has_side_effects=True),
        name="exchange",
    )(sent)


def place_kernel(x_ref, column_ref, down_ref, emb_ref, term_ref, placing_ref, total):
    sources, _, slots, group, share = x_ref.shape
    i, j = pl.program_id(0), pl.program_id(1)

    @pl.when((i == 0) & (j == 0))
    def _():
        columns = lax.broadcasted_iota(jnp.int32, placing_ref.shape, 1)
        placing_ref[...] = jnp.where(column_ref[...] == columns, 1.0, 0.0).astype(jnp.bfloat16)

    x = x_ref[...].reshape(sources * slots * group, share)
    emb = lax.dot_general(
        x, placing_ref[...], (((0,), (0,)), ((), ())), preferred_element_type=jnp.float32
    ).astype(jnp.bfloat16)
    emb_ref[...] = emb
    part = jnp.dot(emb, down_ref[0], preferred_element_type=jnp.float32)

    @pl.when(j == 0)
    def _():
        total[...] = part

    @pl.when(j > 0)
    def _():
        total[...] += part

    @pl.when(j == pl.num_programs(1) - 1)
    def _():
        term_ref[...] = total[...].astype(jnp.bfloat16)


def place(received, column, cross_down):
    sources, groups, slots, emb_local, share = received.shape
    _, width, rank = cross_down.shape
    cols = sources * slots * GROUP
    return pl.pallas_call(
        place_kernel,
        out_shape=(
            jax.ShapeDtypeStruct((groups * share, width), jnp.bfloat16),
            jax.ShapeDtypeStruct((groups * share, rank), jnp.bfloat16),
        ),
        grid=(groups, emb_local // GROUP),
        in_specs=[
            pl.BlockSpec((sources, 1, slots, GROUP, share), lambda i, j: (0, i, 0, j, 0)),
            pl.BlockSpec((cols, 1), lambda i, j: (0, 0)),
            pl.BlockSpec((1, cols, rank), lambda i, j: (0, j, 0)),
        ],
        out_specs=(
            pl.BlockSpec((share, cols), lambda i, j: (i, j)),
            pl.BlockSpec((share, rank), lambda i, j: (i, 0)),
        ),
        scratch_shapes=[
            pltpu.VMEM((cols, cols), jnp.bfloat16),
            pltpu.VMEM((share, rank), jnp.float32),
        ],
        compiler_params=pltpu.CompilerParams(vmem_limit_bytes=40 * 2**20),
        name="place",
    )(received, column, cross_down)


PIECES = 4


def reduce_kernel(groups, term_ref, low_ref, near_in, held, far_in, *sems):
    b, m = lax.axis_index("batch"), lax.axis_index("mp")
    near_send, near_recv, far_send, far_recv, back_send, back_recv = sems
    near = (b, partner(m, 1, groups))
    far = [(b, partner(m, 1 << (s + 1), groups)) for s in range(far_in.shape[0])]
    half = term_ref.shape[0] // 2
    piece = half // PIECES
    core = m % 2

    def rows(who, k):
        return pl.ds(pl.multiple_of(who * half + k * piece, piece), piece)

    barrier = pltpu.get_barrier_semaphore()
    for peer in [near] + far:
        pl.semaphore_signal(barrier, inc=1, device_id=peer, device_id_type=MESH)
    pl.semaphore_wait(barrier, 1 + len(far))

    def send(src, dst, send_sem, recv_sem, peer):
        copy = pltpu.make_async_remote_copy(
            src_ref=src,
            dst_ref=dst,
            send_sem=send_sem,
            recv_sem=recv_sem,
            device_id=peer,
            device_id_type=MESH,
        )
        copy.start()
        return copy

    sent = []
    going = [
        send(term_ref.at[rows(1 - core, k)], near_in.at[k], near_send.at[k], near_recv.at[k], near)
        for k in range(PIECES)
    ]
    for s in range(len(far) + 1):
        arriving, going = going, []
        for k in range(PIECES):
            arriving[k].wait_recv()
            if s == 0:
                mine, other = term_ref[rows(core, k)], near_in[k]
            else:
                mine, other = held[s - 1, k], far_in[s - 1, k]
            total = (mine.astype(jnp.float32) + other.astype(jnp.float32)).astype(jnp.bfloat16)
            if s < len(far):
                held[s, k] = total
                going.append(
                    send(
                        held.at[s, k], far_in.at[s, k], far_send.at[s, k], far_recv.at[s, k], far[s]
                    )
                )
            else:
                place = rows(core, k)
                low_ref[place] = total
                going.append(
                    send(low_ref.at[place], low_ref.at[place], back_send.at[k], back_recv.at[k], near)
                )
        sent += arriving
    for copy in going:
        copy.wait_recv()
    for copy in sent + going:
        copy.wait_send()


def reduce_over_mp(term):
    groups = lax.axis_size("mp")
    stages = groups.bit_length() - 2
    rows, rank = term.shape
    block = (PIECES, rows // 2 // PIECES, rank)
    dma = pltpu.SemaphoreType.DMA
    return pl.pallas_call(
        functools.partial(reduce_kernel, groups),
        out_shape=jax.ShapeDtypeStruct(term.shape, term.dtype),
        in_specs=[pl.BlockSpec(memory_space=pltpu.VMEM)],
        out_specs=pl.BlockSpec(memory_space=pltpu.VMEM),
        scratch_shapes=[
            pltpu.VMEM(block, term.dtype),
            pltpu.VMEM((stages,) + block, term.dtype),
            pltpu.VMEM((stages,) + block, term.dtype),
            dma((PIECES,)),
            dma((PIECES,)),
            dma((stages, PIECES)),
            dma((stages, PIECES)),
            dma((PIECES,)),
            dma((PIECES,)),
        ],
        compiler_params=pltpu.CompilerParams(
            collective_id=1, has_side_effects=True, vmem_limit_bytes=24 * 2**20
        ),
        name="reduce",
    )(term)


def per_device(lookup_ids, table_feature, tables, cross_down, cross_up, cross_bias):
    slots_local = tables.shape[0]
    feats = table_feature.shape[0]
    sources = lax.axis_size("batch")
    groups = lax.axis_size("mp")
    examples_local = lookup_ids.shape[1] // sources
    share = examples_local // groups
    start = lax.axis_index("mp") * share
    by_owner = lookup_ids.reshape(slots_local, sources, examples_local)
    wanted = lax.dynamic_slice_in_dim(by_owner, start, share, 2)
    wanted = wanted.reshape(slots_local * sources * share)
    received = exchange(gather(wanted, tables, sources, groups, share))
    column = (table_feature[:, None] + feats * jnp.arange(GROUP)[None, :]).reshape(-1, 1)
    embedded, term = place(received, column, cross_down)
    embedded_wide = embedded.astype(jnp.float32)
    state = embedded
    for layer in range(len(cross_down)):
        if layer > 0:
            term = jnp.dot(state, cross_down[layer], preferred_element_type=jnp.float32)
            term = term.astype(jnp.bfloat16)
        low = reduce_over_mp(term)
        high = (
            jnp.dot(low, cross_up[layer], preferred_element_type=jnp.float32)
            + cross_bias[layer][None, :]
        )
        state = (embedded_wide * high + state.astype(jnp.float32)).astype(jnp.bfloat16)
    return state


def solution(mesh):
    return jax.shard_map(
        per_device,
        mesh=mesh,
        in_specs=(
            P("batch", None),
            P(),
            P("batch", None, None),
            P(None, "mp", None),
            P(None, None, "mp"),
            P(None, "mp"),
        ),
        out_specs=P("batch", "mp"),
        check_vma=False,
    )
```
